256 devices in a mesh: seq: 64 (over z, y_lo, x), head: 4 (over y_hi, core).
Axes of the slice: x: 4, y: 4 (y_hi: 2, y_lo: 2; y = y_hi * 2 + y_lo), z: 8, core: 2. Of those that a mesh axis runs over, the one named last changes fastest.
Arguments:
- queries: bfloat16 [16384, 32, 128], P('seq', 'head'), may hold values from -6 to 6
- key_vectors: bfloat16 [16384, 4, 128], P(('seq', 'head')), may hold values from -6 to 6
- value_vectors: bfloat16 [16384, 4, 128], P(('seq', 'head')), may hold values from -6 to 6
- out_grad: bfloat16 [16384, 32, 128], P('seq', 'head'), may hold values from -6 to 6
Outputs:
- attended: bfloat16 [16384, 32, 128], P('seq', 'head')
- query_grad: bfloat16 [16384, 32, 128], P('seq', 'head')
- key_grad: bfloat16 [16384, 4, 128], P(('seq', 'head'))
- value_grad: bfloat16 [16384, 4, 128], P(('seq', 'head'))
The draws below stay inside these ranges and needn't reach their ends.
All inputs are finite; a program needn't handle non-finite values.
Results may differ from the reference program's by a relative error of at most 0.035.
Values may be sent and summed in bfloat16 or wider, within the bound.
No kernel may reach another device: no remote copies, remote signals or barrier semaphores. Data moves between devices by JAX's collectives and lax.ppermute only.
A program may use at most 64 MiB of HBM per device.

```python
import math
import jax
import jax.numpy as jnp
from jax import lax

HEAD_DIM = 128
Q_PER_KV = 8
GROUPS = 4
KV_HEADS = 4
Q_HEADS = 32
TOKENS = 16384


def draw_queries(key, part):
    full_shape = (TOKENS, Q_HEADS, HEAD_DIM)
    own_key = jax.random.fold_in(key, 101)
    drawn = jnp.clip(jax.random.normal(own_key, full_shape, jnp.float32), -4.0, 4.0)
    return drawn.astype(jnp.bfloat16)


def draw_key_vectors(key, part):
    full_shape = (TOKENS, KV_HEADS, HEAD_DIM)
    own_key = jax.random.fold_in(key, 202)
    drawn = jnp.clip(jax.random.normal(own_key, full_shape, jnp.float32), -4.0, 4.0)
    return drawn.astype(jnp.bfloat16)


def shard_levels(stream_key, extent, pieces, smallest, top_value):
    factor_of, own = 1.0, jax.random.fold_in(stream_key, 6)
    for position, shards_of in pieces:
        draws = jnp.exp(jax.random.uniform(jax.random.fold_in(own, position), (shards_of,), jnp.float32, smallest / len(pieces), top_value / len(pieces)))
        factor_of = factor_of * jnp.repeat(draws, extent[position] // shards_of).reshape([-1 if axis == position else 1 for axis in range(len(extent))])
    return factor_of


def centred(rng, dims, deviation, reach, cuts=(), kind=jnp.bfloat16):
    values = jax.random.normal(rng, dims, jnp.float32) * deviation
    if len(cuts) > 0:
        values = shard_levels(rng, dims, cuts, -0.22, 0.18) * values
    return jnp.clip(values, min=-reach, max=reach).astype(kind)


def setup_inputs(seed: int = 0) -> dict:
    seeds = jax.random.split(jax.random.key(seed), 5)
    queries = draw_queries(jax.random.fold_in(seeds[4], 71), 0)
    key_vectors = draw_key_vectors(jax.random.fold_in(seeds[4], 71), 0)
    value_vectors = centred(seeds[2], (TOKENS, KV_HEADS, HEAD_DIM), 1.0, 6.0, ((0, 256),))
    out_grad = centred(seeds[3], (TOKENS, Q_HEADS, HEAD_DIM), 1.0, 6.0, ((0, 64), (1, 4)))
    return dict(queries=queries, key_vectors=key_vectors, value_vectors=value_vectors, out_grad=out_grad)


precise = lax.Precision.HIGHEST

def grouped_core(block):
    query_blk, key_blk, value_blk, grad_blk = block
    length = query_blk.shape[0]
    score_scale = 1.0 / math.sqrt(query_blk.shape[2])
    query_f = query_blk.astype(jnp.float32)
    key_f = key_blk.astype(jnp.float32)
    value_f = value_blk.astype(jnp.float32)
    grad_f = grad_blk.astype(jnp.float32)
    causal = jnp.arange(length, dtype=jnp.int32)[:, None] >= jnp.arange(length, dtype=jnp.int32)[None, :]
    scores = jnp.einsum('ihd,td->hit', query_f, key_f, precision=precise) * score_scale
    scores = jnp.where(causal[None], scores, -jnp.inf)
    row_max = lax.optimization_barrier(jnp.max(scores, axis=2))
    log_total = row_max + jnp.log(lax.optimization_barrier(jnp.sum(jnp.exp(scores - row_max[:, :, None]), axis=2)))
    prob_full = jnp.exp(scores - log_total[:, :, None])
    weights = prob_full.astype(jnp.bfloat16)
    attended = jnp.einsum('hit,td->ihd', weights.astype(jnp.float32), value_f, precision=precise).astype(jnp.bfloat16)
    delta_row = jnp.einsum('ihd,ihd->hi', grad_f, attended.astype(jnp.float32), precision=precise)
    prob_grad = jnp.einsum('ihd,td->hit', grad_f, value_f, precision=precise)
    score_grad = (prob_full * (prob_grad - delta_row[:, :, None])).astype(jnp.bfloat16)
    score_f = score_grad.astype(jnp.float32)
    query_grad = (jnp.einsum('hit,td->ihd', score_f, key_f, precision=precise) * score_scale).astype(jnp.bfloat16)
    key_grad = jnp.einsum('hit,ihd->td', score_f, query_f, precision=precise) * score_scale
    value_grad = jnp.einsum('hit,ihd->td', weights.astype(jnp.float32), grad_f, precision=precise)
    return (attended, query_grad, key_grad, value_grad)

def reference(queries, key_vectors, value_vectors, out_grad):
    tok_total = queries.shape[0]
    head_dim = queries.shape[2]
    kv_count = key_vectors.shape[1]
    group_len = tok_total // GROUPS
    half_heads = Q_PER_KV // 2
    attended_all = []
    query_all = []
    key_all = []
    value_all = []
    for kv_index in range(kv_count):
        first_head = kv_index * Q_PER_KV
        key_sum = jnp.zeros((tok_total, head_dim), jnp.float32)
        value_sum = jnp.zeros((tok_total, head_dim), jnp.float32)
        for shifted in range(2):
            offset = shifted * (group_len // 2)
            low_head = first_head + shifted * half_heads
            picked = (queries[:, low_head:low_head + half_heads], key_vectors[:, kv_index], value_vectors[:, kv_index], out_grad[:, low_head:low_head + half_heads])
            rolled = tuple((jnp.roll(member, -offset, axis=0).reshape((GROUPS, group_len) + member.shape[1:]) for member in picked))
            results = lax.map(grouped_core, rolled)
            unrolled = [jnp.roll(member.reshape((tok_total,) + member.shape[2:]), offset, axis=0) for member in results]
            attended_all.append(unrolled[0])
            query_all.append(unrolled[1])
            key_sum = key_sum + unrolled[2]
            value_sum = value_sum + unrolled[3]
        key_all.append(key_sum.astype(jnp.bfloat16))
        value_all.append(value_sum.astype(jnp.bfloat16))
    attended = jnp.concatenate(attended_all, axis=1)
    query_grad = jnp.concatenate(query_all, axis=1)
    key_grad = jnp.stack(key_all, axis=1)
    value_grad = jnp.stack(value_all, axis=1)
    return (attended, query_grad, key_grad, value_grad)
```

```python
import functools
import math

import jax
import jax.numpy as jnp
from jax import lax
from jax.experimental import pallas as pl
from jax.experimental.pallas import tpu as pltpu
from jax.sharding import Mesh, PartitionSpec as P

BLOCK = 256
DIM = 128
HEADS = 8
HALF = 4
NX = 4
SCALE = 1.0 / math.sqrt(DIM)
TO_LOG2 = SCALE * math.log2(math.e)
F32 = jnp.float32
BF16 = jnp.bfloat16
COLUMN = ("ylo", "yhi", "core")


def dot(a, b):
    return jnp.dot(a, b, preferred_element_type=F32)


def causal():
    t = lax.broadcasted_iota(jnp.int32, (BLOCK, BLOCK), 0)
    i = lax.broadcasted_iota(jnp.int32, (BLOCK, BLOCK), 1)
    return t <= i


def slot_of(rank, x):
    return lax.rem(x - lax.rem(rank, NX) + NX, NX) * 2 + lax.div(rank, NX)


def forward_own(place, kv, q_t, acc, top, total):
    x = place[0]
    rank = place[1]

    def tile(slot, diagonal):
        key = kv[slot, :, :DIM]
        value_t = kv[slot, :, DIM:].T
        for h in range(HEADS):
            s = dot(key, q_t[h])
            if diagonal:
                s = jnp.where(causal(), s, -jnp.inf)
                new_top = jnp.max(s, axis=0, keepdims=True)
                w = jnp.exp2((s - new_top) * TO_LOG2)
                total[h : h + 1, :] = jnp.sum(w, axis=0, keepdims=True)
                acc[h] = dot(value_t, w.astype(BF16))
            else:
                old_top = top[h : h + 1, :]
                new_top = jnp.maximum(old_top, jnp.max(s, axis=0, keepdims=True))
                w = jnp.exp2((s - new_top) * TO_LOG2)
                fade = jnp.exp2((old_top - new_top) * TO_LOG2)
                total[h : h + 1, :] = total[h : h + 1, :] * fade + jnp.sum(w, axis=0, keepdims=True)
                acc[h] = acc[h] * fade + dot(value_t, w.astype(BF16))
            top[h : h + 1, :] = new_top

    tile(slot_of(rank, x), True)

    def step(b, carry):
        tile(slot_of(b, x), False)
        return carry

    lax.fori_loop(0, rank, step, 0)


def middle(place, kv, q_t, q, g_t, g, acc, top, total, out_t, log_total, delta, dq_t, dkv, acc2, top2, total2):
    wide = place[2]
    acc2[...] = acc[pl.ds(wide, HALF)]
    for h in range(HALF):
        top2[h : h + 1, :] = top[pl.ds(wide + h, 1), :]
        total2[h : h + 1, :] = total[pl.ds(wide + h, 1), :]

    def forward(b, carry):
        key = kv[b, :, :DIM]
        value_t = kv[b, :, DIM:].T
        for h in range(HALF):
            s = dot(key, q_t[wide + h])
            old_top = top2[h : h + 1, :]
            new_top = jnp.maximum(old_top, jnp.max(s, axis=0, keepdims=True))
            w = jnp.exp2((s - new_top) * TO_LOG2)
            fade = jnp.exp2((old_top - new_top) * TO_LOG2)
            total2[h : h + 1, :] = total2[h : h + 1, :] * fade + jnp.sum(w, axis=0, keepdims=True)
            acc2[h] = acc2[h] * fade + dot(value_t, w.astype(BF16))
            top2[h : h + 1, :] = new_top
        return carry

    lax.fori_loop(0, 2 * NX, forward, 0)

    def finish(h, a, t, l):
        o = (a / l).astype(BF16)
        out_t[h] = o
        log_total[pl.ds(h, 1), :] = t * TO_LOG2 + jnp.log2(l)
        delta[pl.ds(h, 1), :] = jnp.sum(o.astype(F32) * g_t[h].astype(F32), axis=0, keepdims=True)

    narrow = HALF - wide
    for h in range(HALF):
        finish(wide + h, acc2[h], top2[h : h + 1, :], total2[h : h + 1, :])
        finish(
            narrow + h,
            acc[narrow + h],
            top[pl.ds(narrow + h, 1), :],
            total[pl.ds(narrow + h, 1), :],
        )
    dq_t[...] = jnp.zeros_like(dq_t)

    def backward(b, carry):
        key = kv[b, :, :DIM]
        value = kv[b, :, DIM:]
        key_t = key.T
        dk = dv = None
        for h in range(HALF):
            j = wide + h
            s = dot(key, q_t[j])
            prob = jnp.exp2(s * TO_LOG2 - log_total[pl.ds(j, 1), :])
            prob_grad = dot(value, g_t[j])
            ds = (prob * (prob_grad - delta[pl.ds(j, 1), :])).astype(BF16)
            dv_h = dot(prob.astype(BF16), g[j])
            dk_h = dot(ds, q[j])
            dv = dv_h if dv is None else dv + dv_h
            dk = dk_h if dk is None else dk + dk_h
            dq_t[h] += dot(key_t, ds)
        dkv[b, :, :DIM] = (dk * SCALE).astype(BF16)
        dkv[b, :, DIM:] = dv.astype(BF16)
        return carry

    lax.fori_loop(0, 2 * NX, backward, 0)


def backward_own(place, kv, q_t, q, g_t, g, log_total, delta, dq_wide, dq_out, dkv, dq_t):
    x = place[0]
    rank = place[1]
    wide = place[2]
    dq_t[pl.ds(wide, HALF)] = dq_wide[...]
    dq_t[pl.ds(HALF - wide, HALF)] = jnp.zeros((HALF, DIM, BLOCK), F32)

    def tile(slot, diagonal):
        key = kv[slot, :, :DIM]
        value = kv[slot, :, DIM:]
        key_t = key.T
        dk = dv = None
        for h in range(HEADS):
            s = dot(key, q_t[h])
            prob = jnp.exp2(s * TO_LOG2 - log_total[h : h + 1, :])
            if diagonal:
                prob = jnp.where(causal(), prob, 0.0)
            prob_grad = dot(value, g_t[h])
            ds = (prob * (prob_grad - delta[h : h + 1, :])).astype(BF16)
            dv_h = dot(prob.astype(BF16), g[h])
            dk_h = dot(ds, q[h])
            dv = dv_h if dv is None else dv + dv_h
            dk = dk_h if dk is None else dk + dk_h
            dq_t[h] += dot(key_t, ds)
        dkv[slot, :, :DIM] = (dk * SCALE).astype(BF16)
        dkv[slot, :, DIM:] = dv.astype(BF16)

    def step(b, carry):
        tile(slot_of(b, x), False)
        return carry

    lax.fori_loop(0, rank, step, 0)
    tile(slot_of(rank, x), True)

    def blank(b, carry):
        dkv[slot_of(b, x)] = jnp.zeros((BLOCK, 2 * DIM), BF16)
        return carry

    lax.fori_loop(rank + 1, 2 * NX, blank, 0)
    for h in range(HEADS):
        dq_out[h] = (dq_t[h] * SCALE).astype(BF16)


def call(body, outs, ins, scratch=(), flops=1 << 30):
    vmem = pl.BlockSpec(memory_space=pltpu.VMEM)
    smem = pl.BlockSpec(memory_space=pltpu.SMEM)
    return pl.pallas_call(
        body,
        out_shape=outs,
        in_specs=[smem] + [vmem] * (len(ins) - 1),
        out_specs=[vmem] * len(outs),
        scratch_shapes=list(scratch),
        compiler_params=pltpu.CompilerParams(vmem_limit_bytes=40 << 20),
        cost_estimate=pl.CostEstimate(flops=flops, bytes_accessed=4 << 20, transcendentals=1 << 20),
    )(*ins)


def ring(size, by):
    return [(i, (i + by) % size) for i in range(size)]


def from_row(value):
    parts = [value]
    for by in range(1, NX):
        parts.append(lax.ppermute(value, "x", ring(NX, by)))
    return jnp.stack(parts).reshape(2 * NX, BLOCK, 2 * DIM)


def to_row(grads):
    grads = grads.reshape(NX, 2 * BLOCK, 2 * DIM)
    total = grads[0].astype(F32)
    for by in range(1, NX):
        total = total + lax.ppermute(grads[by], "x", ring(NX, -by)).astype(F32)
    return total


def per_device(queries, key_vectors, value_vectors, out_grad):
    x = lax.axis_index("x")
    z = lax.axis_index("z")
    rank = lax.axis_index("ylo") * NX + x
    wide = jnp.where(z % 2 == 0, HALF, 0)
    place = jnp.stack([x, rank, wide]).astype(jnp.int32)

    both = jnp.concatenate([key_vectors, value_vectors], axis=2)
    both = jnp.concatenate([both, both], axis=1)
    home = lax.all_to_all(both, COLUMN, 1, 0, tiled=True)[:, 0, :]
    own = from_row(home)
    before = from_row(lax.ppermute(home, "z", ring(8, 1)))

    q = jnp.transpose(queries, (1, 0, 2))
    q_t = jnp.transpose(queries, (1, 2, 0))
    g = jnp.transpose(out_grad, (1, 0, 2))
    g_t = jnp.transpose(out_grad, (1, 2, 0))

    sds = jax.ShapeDtypeStruct
    acc_shape = sds((HEADS, DIM, BLOCK), F32)
    row_shape = sds((HEADS, BLOCK), F32)
    acc, top, total = call(
        forward_own,
        [acc_shape, row_shape, row_shape],
        [place, own, q_t],
        flops=4 << 30,
    )
    out_t, log_total, delta, dq_wide, dkv_before = call(
        middle,
        [
            sds((HEADS, DIM, BLOCK), BF16),
            row_shape,
            row_shape,
            sds((HALF, DIM, BLOCK), F32),
            sds((2 * NX, BLOCK, 2 * DIM), BF16),
        ],
        [place, before, q_t, q, g_t, g, acc, top, total],
        [
            pltpu.VMEM((HALF, DIM, BLOCK), F32),
            pltpu.VMEM((HALF, BLOCK), F32),
            pltpu.VMEM((HALF, BLOCK), F32),
        ],
        flops=8 << 30,
    )
    row_before = lax.ppermute(to_row(dkv_before).astype(BF16), "z", ring(8, -1))
    dq_t, dkv_own = call(
        backward_own,
        [sds((HEADS, DIM, BLOCK), BF16), sds((2 * NX, BLOCK, 2 * DIM), BF16)],
        [place, own, q_t, q, g_t, g, log_total, delta, dq_wide],
        [pltpu.VMEM((HEADS, DIM, BLOCK), F32)],
        flops=8 << 30,
    )
    row = (to_row(dkv_own) + row_before.astype(F32)).astype(BF16)
    back = lax.all_to_all(row.reshape(8, 64, 2 * DIM), COLUMN, 0, 0, tiled=True)
    back = back.reshape(2, HALF, 64, 2 * DIM).astype(F32)
    back = jnp.transpose(back[0] + back[1], (1, 0, 2)).astype(BF16)
    attended = jnp.transpose(out_t, (2, 0, 1))
    query_grad = jnp.transpose(dq_t, (2, 0, 1))
    return attended, query_grad, back[:, :, :DIM], back[:, :, DIM:]


def solution(mesh):
    inner = Mesh(mesh.devices.reshape(8, 2, NX, 2, 2), ("z", "ylo", "x", "yhi", "core"))
    tokens = ("z", "ylo", "x")
    heads = ("yhi", "core")
    by_head = P(tokens, heads, None)
    by_token = P(tokens + heads, None, None)
    return jax.shard_map(
        per_device,
        mesh=inner,
        in_specs=(by_head, by_token, by_token, by_head),
        out_specs=(by_head, by_head, by_token, by_token),
        check_vma=False,
    )
```

```python
import math

import jax
import jax.numpy as jnp
from jax import lax
from jax.experimental import pallas as pl
from jax.experimental.pallas import tpu as pltpu
from jax.sharding import Mesh, PartitionSpec as P

BLOCK = 256
DIM = 128
HEADS = 8
HALF = 4
NX = 4
RANKS = 8
LIMIT = 63 << 20
SCALE = 1.0 / math.sqrt(DIM)
TO_LOG2 = SCALE * math.log2(math.e)
F32 = jnp.float32
BF16 = jnp.bfloat16
PLANE = ("ylo", "x", "yhi", "core")


def dot(a, b):
    return jnp.dot(a, b, preferred_element_type=F32)


def causal():
    t = lax.broadcasted_iota(jnp.int32, (BLOCK, BLOCK), 0)
    i = lax.broadcasted_iota(jnp.int32, (BLOCK, BLOCK), 1)
    return t <= i


def forward_tile(kv, heads, q_t, acc, top, total, scores, first, diagonal):
    key = kv[:, :DIM]
    value_t = kv[:, DIM:].T
    for h in range(heads):
        scores[h] = dot(key, q_t[h])
    for h in range(heads):
        s = scores[h]
        if diagonal:
            s = jnp.where(causal(), s, -jnp.inf)
        new_top = jnp.max(s, axis=0, keepdims=True)
        if first:
            w = jnp.exp2((s - new_top) * TO_LOG2)
            total[h : h + 1, :] = jnp.sum(w, axis=0, keepdims=True)
            acc[h] = dot(value_t, w.astype(BF16))
        else:
            old_top = top[h : h + 1, :]
            new_top = jnp.maximum(old_top, new_top)
            w = jnp.exp2((s - new_top) * TO_LOG2)
            fade = jnp.exp2((old_top - new_top) * TO_LOG2)
            total[h : h + 1, :] = total[h : h + 1, :] * fade + jnp.sum(w, axis=0, keepdims=True)
            acc[h] = acc[h] * fade + dot(value_t, w.astype(BF16))
        top[h : h + 1, :] = new_top


def backward_tile(kv, heads, q_t, q, g_t, g, log_total, delta, dq_t, scores, grads, probs, ds, diagonal):
    key = kv[:, :DIM]
    value = kv[:, DIM:]
    key_t = key.T
    for h in range(heads):
        scores[h] = dot(key, q_t[h])
        grads[h] = dot(value, g_t[h])
    for h in range(heads):
        prob = jnp.exp2(scores[h] * TO_LOG2 - log_total[h : h + 1, :])
        if diagonal:
            prob = jnp.where(causal(), prob, 0.0)
        probs[h] = prob.astype(BF16)
        ds[h] = (prob * (grads[h] - delta[h : h + 1, :])).astype(BF16)
    dv = dot(probs[0], g[0])
    dk = dot(ds[0], q[0])
    for h in range(1, heads):
        dv = dv + dot(probs[h], g[h])
        dk = dk + dot(ds[h], q[h])
    for h in range(heads):
        dq_t[h] += dot(key_t, ds[h])
    return jnp.concatenate([dk * SCALE, dv], axis=1)


def far_forward(place, kv_far, q_t_far, part_far, log_part, kv, q_t, acc, part, top, total, scores, sems):
    loads = [pltpu.make_async_copy(q_t_far, q_t, sems.at[0]), pltpu.make_async_copy(kv_far, kv, sems.at[1])]
    for load in loads:
        load.start()
    for load in loads:
        load.wait()
    forward_tile(kv[0], HALF, q_t, acc, top, total, scores, True, False)

    def forward(b, carry):
        forward_tile(kv[b], HALF, q_t, acc, top, total, scores, False, False)
        return carry

    lax.fori_loop(1, kv.shape[0], forward, 0)
    for h in range(HALF):
        part[h] = (acc[h] / total[h : h + 1, :]).astype(BF16)
    log_part[...] = top[...] * TO_LOG2 + jnp.log2(total[...])
    store = pltpu.make_async_copy(part, part_far, sems.at[2])
    store.start()
    store.wait()


def finish(o, g_t):
    rounded = o.astype(BF16)
    return rounded, jnp.sum(rounded.astype(F32) * g_t.astype(F32), axis=0, keepdims=True)


def own_forward(
    place, kv_far, q_t_far, g_t_far,
    out_far, own_wide_far, log_narrow, delta_narrow, log_wide,
    kv, q_t, g_t, acc, out, own_wide, top, total, scores, sems,
):
    rank = place[0]
    wide = place[1]
    narrow = HALF - wide
    loads = [
        pltpu.make_async_copy(q_t_far, q_t, sems.at[0]),
        pltpu.make_async_copy(kv_far, kv, sems.at[1]),
        pltpu.make_async_copy(g_t_far.at[pl.ds(narrow, HALF)], g_t, sems.at[2]),
    ]
    for load in loads:
        load.start()
    for load in loads[:2]:
        load.wait()
    forward_tile(kv[rank], HEADS, q_t, acc, top, total, scores, True, True)

    def forward(b, carry):
        forward_tile(kv[b], HEADS, q_t, acc, top, total, scores, False, False)
        return carry

    lax.fori_loop(0, rank, forward, 0)
    for h in range(HALF):
        own_wide[h] = acc[wide + h] / total[pl.ds(wide + h, 1), :]
        log_wide[h : h + 1, :] = top[pl.ds(wide + h, 1), :] * TO_LOG2 + jnp.log2(total[pl.ds(wide + h, 1), :])
    store_wide = pltpu.make_async_copy(own_wide, own_wide_far, sems.at[3])
    store_wide.start()
    loads[2].wait()
    for h in range(HALF):
        sum_h = total[pl.ds(narrow + h, 1), :]
        out[h], delta_narrow[h : h + 1, :] = finish(acc[narrow + h] / sum_h, g_t[h])
        log_narrow[h : h + 1, :] = top[pl.ds(narrow + h, 1), :] * TO_LOG2 + jnp.log2(sum_h)
    store_out = pltpu.make_async_copy(out, out_far.at[pl.ds(narrow, HALF)], sems.at[4])
    store_out.start()
    store_wide.wait()
    store_out.wait()


def merge(
    place, own_wide_far, part_far, g_t_far, log_narrow, delta_narrow, log_wide, log_part, out_in,
    out_far, log_total, delta, stats,
    own_wide, part, g_t, out, sems,
):
    wide = place[1]
    narrow = HALF - wide
    wides = pl.ds(wide, HALF)
    loads = [
        pltpu.make_async_copy(own_wide_far, own_wide, sems.at[0]),
        pltpu.make_async_copy(part_far, part, sems.at[1]),
        pltpu.make_async_copy(g_t_far.at[wides], g_t, sems.at[2]),
    ]
    for load in loads:
        load.start()
    for load in loads:
        load.wait()
    for h in range(HALF):
        a = log_wide[h : h + 1, :]
        b = log_part[h : h + 1, :]
        top = jnp.maximum(a, b)
        log_h = top + jnp.log2(jnp.exp2(a - top) + jnp.exp2(b - top))
        out[h], delta_h = finish(
            own_wide[h] * jnp.exp2(a - log_h) + part[h].astype(F32) * jnp.exp2(b - log_h), g_t[h]
        )
        stats[h : h + 1, :] = log_h
        stats[HALF + h : HALF + h + 1, :] = delta_h
        log_total[pl.ds(wide + h, 1), :] = log_h
        delta[pl.ds(wide + h, 1), :] = delta_h
        log_total[pl.ds(narrow + h, 1), :] = log_narrow[h : h + 1, :]
        delta[pl.ds(narrow + h, 1), :] = delta_narrow[h : h + 1, :]
    store = pltpu.make_async_copy(out, out_far.at[wides], sems.at[3])
    store.start()
    store.wait()


def own_backward(
    place, kv_far, q_t_far, q_far, g_t_far, g_far, log_total, delta,
    dq_far, dkv_far,
    kv, q_t, q, g_t, g, dq_t, dkv, scores, grads, probs, ds, sems, tile_sems,
):
    rank = place[0]
    loads = [
        pltpu.make_async_copy(far, near, sems.at[i])
        for i, (far, near) in enumerate([(q_t_far, q_t), (kv_far, kv), (g_t_far, g_t), (g_far, g), (q_far, q)])
    ]
    for load in loads:
        load.start()

    def store(b):
        return pltpu.make_async_copy(dkv.at[b], dkv_far.at[b], tile_sems.at[b])

    def blank(b, carry):
        dkv[b] = jnp.zeros((BLOCK, 2 * DIM), F32)
        store(b).start()
        return carry

    lax.fori_loop(rank + 1, RANKS, blank, 0)
    dq_t[...] = jnp.zeros_like(dq_t)
    for load in loads:
        load.wait()

    def tile(b, diagonal):
        dkv[b] = backward_tile(
            kv[b], HEADS, q_t, q, g_t, g, log_total, delta, dq_t, scores, grads, probs, ds, diagonal
        )
        store(b).start()

    tile(rank, True)

    def backward(b, carry):
        tile(b, False)
        return carry

    lax.fori_loop(0, rank, backward, 0)
    dq_store = pltpu.make_async_copy(dq_t, dq_far, sems.at[5])
    dq_store.start()
    for b in range(RANKS):
        store(b).wait()
    dq_store.wait()


def far_backward(
    place, kv_far, q_t_far, q_far, g_t_far, g_far, stats, dkv_own_far,
    dq_far, dkv_far,
    kv, q_t, q, g_t, g, dkv_own, dq_t, dq, dkv, log_total, delta, scores, grads, probs, ds, sems, tile_sems,
):
    tiles = kv.shape[0]
    loads = [
        pltpu.make_async_copy(far, near, sems.at[i])
        for i, (far, near) in enumerate(
            [(q_t_far, q_t), (kv_far, kv), (g_t_far, g_t), (g_far, g), (q_far, q), (dkv_own_far, dkv_own)]
        )
    ]
    for load in loads:
        load.start()
    log_total[...] = stats[:HALF, :]
    delta[...] = stats[HALF:, :]
    dq_t[...] = jnp.zeros_like(dq_t)
    for load in loads:
        load.wait()

    def store(b):
        return pltpu.make_async_copy(dkv.at[b], dkv_far.at[b], tile_sems.at[b])

    def backward(b, carry):
        dkv[b] = (
            backward_tile(kv[b], HALF, q_t, q, g_t, g, log_total, delta, dq_t, scores, grads, probs, ds, False)
            + dkv_own[b]
        ).astype(BF16)
        store(b).start()
        return carry

    lax.fori_loop(0, tiles, backward, 0)
    dq[...] = (dq_t[...] * SCALE).astype(BF16)
    dq_store = pltpu.make_async_copy(dq, dq_far, sems.at[6])
    dq_store.start()
    for b in range(tiles):
        store(b).wait()
    dq_store.wait()


FAR = pl.BlockSpec(memory_space=pltpu.HBM)
NEAR = pl.BlockSpec(memory_space=pltpu.VMEM)


def call(body, outs, ins, scratch, sems, flops, aliases=None):
    return pl.pallas_call(
        body,
        out_shape=[jax.ShapeDtypeStruct(s, t) for s, t, _ in outs],
        in_specs=[pl.BlockSpec(memory_space=pltpu.SMEM)] + [spec for _, spec in ins[1:]],
        out_specs=[spec for _, _, spec in outs],
        scratch_shapes=[pltpu.VMEM(s, t) for s, t in scratch] + [pltpu.SemaphoreType.DMA((n,)) for n in sems],
        input_output_aliases=aliases or {},
        compiler_params=pltpu.CompilerParams(vmem_limit_bytes=LIMIT),
        cost_estimate=pl.CostEstimate(flops=flops, bytes_accessed=4 << 20, transcendentals=1 << 20),
    )(*[a for a, _ in ins])


def ring(size, by):
    return [(i, (i + by) % size) for i in range(size)]


def spread(block):
    many = jnp.broadcast_to(block[None], (RANKS,) + block.shape).reshape((4 * RANKS,) + block.shape[1:])
    got = lax.all_to_all(many, PLANE, 0, 0, tiled=True)
    return got.reshape(RANKS, BLOCK, 2 * DIM)


def collect(grads):
    got = lax.all_to_all(grads.reshape(4 * RANKS, 64, 2 * DIM), PLANE, 0, 0, tiled=True)
    return jnp.sum(got.reshape(RANKS, 4, 64, 2 * DIM).astype(F32), axis=0)


def per_device(queries, key_vectors, value_vectors, out_grad):
    rank = lax.axis_index("ylo") * NX + lax.axis_index("x")
    wide = jnp.where(lax.axis_index("z") % 2 == 0, HALF, 0)
    place = jnp.stack([rank, wide]).astype(jnp.int32)

    block = jnp.transpose(jnp.concatenate([key_vectors, value_vectors], axis=2), (1, 0, 2))
    planes = lax.axis_size("z")
    planes = lax.axis_size("z")
    own = spread(block)

    def widest(a, heads):
        return jnp.where(wide == HALF, a[:, heads + HALF : heads + 2 * HALF], a[:, heads : heads + HALF])

    sent = jnp.concatenate([widest(queries, 0), widest(out_grad, 0)], axis=1)
    far = lax.ppermute(sent, "z", ring(planes, -1))
    q = jnp.transpose(queries, (1, 0, 2))
    q_t = jnp.transpose(queries, (1, 2, 0))
    g = jnp.transpose(out_grad, (1, 0, 2))
    g_t = jnp.transpose(out_grad, (1, 2, 0))
    q_far = jnp.transpose(far[:, :HALF], (1, 0, 2))
    q_t_far = jnp.transpose(far[:, :HALF], (1, 2, 0))
    g_far = jnp.transpose(far[:, HALF:], (1, 0, 2))
    g_t_far = jnp.transpose(far[:, HALF:], (1, 2, 0))

    full_t = (HEADS, DIM, BLOCK)
    full = (HEADS, BLOCK, DIM)
    half_t = (HALF, DIM, BLOCK)
    half = (HALF, BLOCK, DIM)
    rows = (HEADS, BLOCK)
    few = (HALF, BLOCK)
    square = (HEADS, BLOCK, BLOCK)
    kv_shape = (RANKS, BLOCK, 2 * DIM)
    tile = 2 * BLOCK
    tiled = (RANKS * BLOCK // tile, tile, 2 * DIM)
    tall = (HALF, tile, BLOCK)
    part, log_part = call(
        far_forward,
        [(half_t, BF16, FAR), (few, F32, NEAR)],
        [(place, None), (own.reshape(tiled), FAR), (q_t_far, FAR)],
        [(tiled, BF16), (half_t, BF16), (half_t, F32), (half_t, BF16), (few, F32), (few, F32), (tall, F32)],
        [3],
        4 << 30,
    )
    part = lax.ppermute(part, "z", ring(planes, 1))
    log_part = lax.ppermute(log_part, "z", ring(planes, 1))
    out_t, own_wide, log_narrow, delta_narrow, log_wide = call(
        own_forward,
        [(full_t, BF16, FAR), (half_t, F32, FAR), (few, F32, NEAR), (few, F32, NEAR), (few, F32, NEAR)],
        [(place, None), (own, FAR), (q_t, FAR), (g_t, FAR)],
        [
            (kv_shape, BF16), (full_t, BF16), (half_t, BF16), (full_t, F32), (half_t, BF16), (half_t, F32),
            (rows, F32), (rows, F32), (square, F32),
        ],
        [5],
        8 << 30,
    )
    out_t, log_total, delta, stats = call(
        merge,
        [(full_t, BF16, FAR), (rows, F32, NEAR), (rows, F32, NEAR), (rows, F32, NEAR)],
        [
            (place, None), (own_wide, FAR), (part, FAR), (g_t, FAR), (log_narrow, NEAR), (delta_narrow, NEAR),
            (log_wide, NEAR), (log_part, NEAR), (out_t, FAR),
        ],
        [(half_t, F32), (half_t, BF16), (half_t, BF16), (half_t, BF16)],
        [4],
        1 << 20,
        {8: 0},
    )
    stats_far = lax.ppermute(stats, "z", ring(planes, -1))
    dq_t, dkv = call(
        own_backward,
        [(full_t, F32, FAR), (kv_shape, F32, FAR)],
        [
            (place, None), (own, FAR), (q_t, FAR), (q, FAR), (g_t, FAR), (g, FAR),
            (log_total, NEAR), (delta, NEAR),
        ],
        [
            (kv_shape, BF16), (full_t, BF16), (full, BF16), (full_t, BF16), (full, BF16),
            (full_t, F32), (kv_shape, F32), (square, F32), (square, F32), (square, BF16), (square, BF16),
        ],
        [6, RANKS],
        16 << 30,
    )
    dq_far, dkv = call(
        far_backward,
        [(half_t, BF16, FAR), (tiled, BF16, FAR)],
        [
            (place, None), (own.reshape(tiled), FAR), (q_t_far, FAR), (q_far, FAR), (g_t_far, FAR), (g_far, FAR),
            (stats_far, NEAR), (dkv.reshape(tiled), FAR),
        ],
        [
            (tiled, BF16), (half_t, BF16), (half, BF16), (half_t, BF16), (half, BF16), (tiled, F32),
            (half_t, F32), (half_t, BF16), (tiled, BF16), (few, F32), (few, F32),
            (tall, F32), (tall, F32), (tall, BF16), (tall, BF16),
        ],
        [7, RANKS * BLOCK // tile],
        8 << 30,
    )
    dq_back = lax.ppermute(dq_far, "z", ring(planes, 1)).astype(F32)
    back = jnp.transpose(collect(dkv).astype(BF16), (1, 0, 2))
    attended = jnp.transpose(out_t, (2, 0, 1))
    high = wide == HALF
    low_part = dq_t[:HALF] * SCALE + jnp.where(high, 0.0, dq_back)
    high_part = dq_t[HALF:] * SCALE + jnp.where(high, dq_back, 0.0)
    query_grad = jnp.transpose(jnp.concatenate([low_part, high_part], axis=0).astype(BF16), (2, 0, 1))
    return attended, query_grad, back[:, :, :DIM], back[:, :, DIM:]


def solution(mesh):
    inner = Mesh(mesh.devices.reshape(8, 2, NX, 2, 2), ("z", "ylo", "x", "yhi", "core"))
    tokens = ("z", "ylo", "x")
    heads = ("yhi", "core")
    by_head = P(tokens, heads, None)
    by_token = P(tokens + heads, None, None)
    return jax.shard_map(
        per_device,
        mesh=inner,
        in_specs=(by_head, by_token, by_token, by_head),
        out_specs=(by_head, by_head, by_token, by_token),
        check_vma=False,
    )
```

```python
import math

import jax
import jax.numpy as jnp
from jax import lax
from jax.experimental import pallas as pl
from jax.experimental.pallas import tpu as pltpu
from jax.sharding import Mesh, PartitionSpec as P

BLOCK = 256
DIM = 128
HEADS = 8
HALF = 4
NX = 4
RANKS = 8
EXTRA = 16
LIMIT = 63 << 20
SCALE = 1.0 / math.sqrt(DIM)
TO_LOG2 = SCALE * math.log2(math.e)
F32 = jnp.float32
BF16 = jnp.bfloat16
PLANE = ("ylo", "x", "yhi", "core")


def dot(a, b):
    return jnp.dot(a, b, preferred_element_type=F32)


def causal():
    t = lax.broadcasted_iota(jnp.int32, (BLOCK, BLOCK), 0)
    i = lax.broadcasted_iota(jnp.int32, (BLOCK, BLOCK), 1)
    return t <= i


def forward_tile(kv, lo, hi, q_t, acc, top, total, scores, first, masked):
    key = kv[:, :DIM]
    value_t = kv[:, DIM:].T
    for h in range(lo, hi):
        scores[h] = dot(key, q_t[h])
    for h in range(lo, hi):
        s = scores[h]
        if h < masked:
            s = jnp.where(causal(), s, -jnp.inf)
        new_top = jnp.max(s, axis=0, keepdims=True)
        if first:
            w = jnp.exp2((s - new_top) * TO_LOG2)
            total[h : h + 1, :] = jnp.sum(w, axis=0, keepdims=True)
            acc[h] = dot(value_t, w.astype(BF16))
        else:
            old_top = top[h : h + 1, :]
            new_top = jnp.maximum(old_top, new_top)
            w = jnp.exp2((s - new_top) * TO_LOG2)
            fade = jnp.exp2((old_top - new_top) * TO_LOG2)
            total[h : h + 1, :] = total[h : h + 1, :] * fade + jnp.sum(w, axis=0, keepdims=True)
            acc[h] = acc[h] * fade + dot(value_t, w.astype(BF16))
        top[h : h + 1, :] = new_top


def backward_tile(kv, lo, hi, q_t, q, g_t, g, log_total, delta, dq_t, scores, grads, probs, ds, masked):
    key = kv[:, :DIM]
    value = kv[:, DIM:]
    key_t = key.T
    for h in range(lo, hi):
        scores[h] = dot(key, q_t[h])
        grads[h] = dot(value, g_t[h])
    for h in range(lo, hi):
        prob = jnp.exp2(scores[h] * TO_LOG2 - log_total[h : h + 1, :])
        if h < masked:
            prob = jnp.where(causal(), prob, 0.0)
        probs[h] = prob.astype(BF16)
        ds[h] = (prob * (grads[h] - delta[h : h + 1, :])).astype(BF16)
    dv = dot(probs[lo], g[lo])
    dk = dot(ds[lo], q[lo])
    for h in range(lo + 1, hi):
        dv = dv + dot(probs[h], g[h])
        dk = dk + dot(ds[h], q[h])
    for h in range(lo, hi):
        dq_t[h] += dot(key_t, ds[h])
    return jnp.concatenate([dk * SCALE, dv], axis=1)


def finish(o, g_t):
    rounded = o.astype(BF16)
    return rounded, jnp.sum(rounded.astype(F32) * g_t.astype(F32), axis=0, keepdims=True)


def pack(o, log):
    row = lax.broadcasted_iota(jnp.int32, (EXTRA, BLOCK), 0)
    first = log.astype(BF16).astype(F32)
    second = (log - first).astype(BF16).astype(F32)
    third = log - first - second
    tail = jnp.where(row == 0, first, jnp.where(row == 1, second, jnp.where(row == 2, third, 0.0)))
    return jnp.concatenate([o.astype(BF16), tail.astype(BF16)], axis=0)


def log_of(packed):
    return jnp.sum(packed[DIM:].astype(F32), axis=0, keepdims=True)


def merged(a, b):
    log_a = log_of(a)
    log_b = log_of(b)
    top = jnp.maximum(log_a, log_b)
    log = top + jnp.log2(jnp.exp2(log_a - top) + jnp.exp2(log_b - top))
    return a[:DIM].astype(F32) * jnp.exp2(log_a - log) + b[:DIM].astype(F32) * jnp.exp2(log_b - log), log


def start_all(pairs, sems):
    copies = [pltpu.make_async_copy(a, b, sems.at[i]) for i, (a, b) in enumerate(pairs)]
    for copy in copies:
        copy.start()
    return copies


def wait_all(copies):
    for copy in copies:
        copy.wait()


def forward(
    place, kv_in, q_t_in, q_t_next_in, g_t_in,
    out_out, mine_out, next_out, log_narrow, delta_narrow,
    kv, q_t, g_t, acc, out, mine, nexts, top, total, scores, sems, out_sems,
):
    rank = place[0]
    wide = place[1]
    narrow = HALF - wide
    loads = start_all(
        [
            (q_t_in, q_t.at[pl.ds(0, HEADS)]),
            (q_t_next_in, q_t.at[pl.ds(HEADS, HALF)]),
            (kv_in, kv),
            (g_t_in.at[pl.ds(narrow, HALF)], g_t),
        ],
        sems,
    )
    wait_all(loads[:3])
    every = HEADS + HALF
    forward_tile(kv[rank], 0, every, q_t, acc, top, total, scores, True, HEADS)

    def below(b, carry):
        forward_tile(kv[b], 0, every, q_t, acc, top, total, scores, False, 0)
        return carry

    def above(b, carry):
        forward_tile(kv[b], HEADS, every, q_t, acc, top, total, scores, False, 0)
        return carry

    lax.fori_loop(0, rank, below, 0)
    lax.fori_loop(rank + 1, RANKS, above, 0)

    def result(n):
        total_n = total[pl.ds(n, 1), :]
        return acc[n] / total_n, top[pl.ds(n, 1), :] * TO_LOG2 + jnp.log2(total_n)

    for h in range(HALF):
        nexts[h] = pack(*result(HEADS + h))
        mine[h] = pack(*result(wide + h))
    stores = start_all([(nexts, next_out), (mine, mine_out)], out_sems)
    loads[3].wait()
    for h in range(HALF):
        o, log_h = result(narrow + h)
        out[h], delta_narrow[h : h + 1, :] = finish(o, g_t[h])
        log_narrow[h : h + 1, :] = log_h
    last = pltpu.make_async_copy(out, out_out.at[pl.ds(narrow, HALF)], out_sems.at[2])
    last.start()
    wait_all(stores)
    last.wait()


def backward_narrow(
    place, kv_in, q_t_in, q_in, g_t_in, g_in, log_narrow, delta_narrow,
    dq_out, dkv_out,
    kv, q_t, q, g_t, g, dq_t, dq, dkv, scores, grads, probs, ds, sems, tile_sems,
):
    rank = place[0]
    part = pl.ds(HALF - place[1], HALF)
    loads = start_all(
        [(q_t_in.at[part], q_t), (kv_in, kv), (g_t_in.at[part], g_t), (g_in.at[part], g), (q_in.at[part], q)],
        sems,
    )
    dq_t[...] = jnp.zeros_like(dq_t)
    wait_all(loads)

    def store(b):
        return pltpu.make_async_copy(dkv.at[b], dkv_out.at[b], tile_sems.at[b])

    def tile(b, masked):
        dkv[b] = backward_tile(
            kv[b], 0, HALF, q_t, q, g_t, g, log_narrow, delta_narrow, dq_t, scores, grads, probs, ds, masked
        )
        store(b).start()

    tile(rank, HALF)

    def below(b, carry):
        tile(b, 0)
        return carry

    lax.fori_loop(0, rank, below, 0)
    dq[...] = (dq_t[...] * SCALE).astype(BF16)
    last = pltpu.make_async_copy(dq, dq_out, sems.at[5])
    last.start()

    def settle(b, carry):
        store(b).wait()
        return carry

    lax.fori_loop(0, rank + 1, settle, 0)
    last.wait()


def backward_wide(
    place, kv_in, q_t_in, q_in, g_t_in, g_in, q_t_next_in, q_next_in, g_t_next_in, g_next_in,
    mine_in, before_in, next_in, after_in, dkv_narrow_in, out_in,
    out_out, dq_out, dq_next_out, dkv_out,
    kv, q_t, q, g_t, g, mine, before, nexts, after, dkv_narrow, out, dq_t, dq, dkv, log_total, delta,
    scores, grads, probs, ds, sems, out_sems, tile_sems,
):
    rank = place[0]
    part = pl.ds(place[1], HALF)
    first = pl.ds(0, HALF)
    second = pl.ds(HALF, HALF)
    loads = start_all(
        [
            (mine_in, mine), (before_in, before), (g_t_in.at[part], g_t.at[first]),
            (next_in, nexts), (after_in, after), (g_t_next_in, g_t.at[second]),
            (q_t_in.at[part], q_t.at[first]), (q_t_next_in, q_t.at[second]), (kv_in, kv),
            (g_in.at[part], g.at[first]), (g_next_in, g.at[second]),
            (q_in.at[part], q.at[first]), (q_next_in, q.at[second]), (dkv_narrow_in, dkv_narrow),
        ],
        sems,
    )
    dq_t[...] = jnp.zeros_like(dq_t)
    wait_all(loads[:6])
    for h in range(HALF):
        o, log_h = merged(mine[h], before[h])
        out[h], delta[h : h + 1, :] = finish(o, g_t[h])
        log_total[h : h + 1, :] = log_h
        n = HALF + h
        o, log_h = merged(after[h], nexts[h])
        _, delta[n : n + 1, :] = finish(o, g_t[n])
        log_total[n : n + 1, :] = log_h
    out_store = pltpu.make_async_copy(out, out_out.at[part], out_sems.at[0])
    out_store.start()
    wait_all(loads[6:])

    def store(b):
        return pltpu.make_async_copy(dkv.at[b], dkv_out.at[b], tile_sems.at[b])

    def tile(b, lo, masked):
        grad = backward_tile(
            kv[b], lo, HEADS, q_t, q, g_t, g, log_total, delta, dq_t, scores, grads, probs, ds, masked
        )
        if lo == 0:
            grad = grad + dkv_narrow[b]
        dkv[b] = grad.astype(BF16)
        store(b).start()

    tile(rank, 0, HALF)

    def below(b, carry):
        tile(b, 0, 0)
        return carry

    def above(b, carry):
        tile(b, HALF, 0)
        return carry

    lax.fori_loop(0, rank, below, 0)
    lax.fori_loop(rank + 1, RANKS, above, 0)
    dq[...] = (dq_t[...] * SCALE).astype(BF16)
    dq_store = pltpu.make_async_copy(dq.at[first], dq_out, out_sems.at[1])
    dq_next_store = pltpu.make_async_copy(dq.at[second], dq_next_out, out_sems.at[2])
    dq_store.start()
    dq_next_store.start()
    for b in range(RANKS):
        store(b).wait()
    out_store.wait()
    dq_store.wait()
    dq_next_store.wait()


FAR = pl.BlockSpec(memory_space=pltpu.HBM)
NEAR = pl.BlockSpec(memory_space=pltpu.VMEM)


def call(body, outs, ins, scratch, sems, flops, aliases=None):
    return pl.pallas_call(
        body,
        out_shape=[jax.ShapeDtypeStruct(s, t) for s, t, _ in outs],
        in_specs=[pl.BlockSpec(memory_space=pltpu.SMEM)] + [spec for _, spec in ins[1:]],
        out_specs=[spec for _, _, spec in outs],
        scratch_shapes=[pltpu.VMEM(s, t) for s, t in scratch] + [pltpu.SemaphoreType.DMA((n,)) for n in sems],
        input_output_aliases=aliases or {},
        compiler_params=pltpu.CompilerParams(vmem_limit_bytes=LIMIT),
        cost_estimate=pl.CostEstimate(flops=flops, bytes_accessed=4 << 20, transcendentals=1 << 20),
    )(*[a for a, _ in ins])


def ring(size, by):
    return [(i, (i + by) % size) for i in range(size)]


def spread(block):
    many = jnp.broadcast_to(block[None], (RANKS,) + block.shape).reshape((4 * RANKS,) + block.shape[1:])
    got = lax.all_to_all(many, PLANE, 0, 0, tiled=True)
    return got.reshape(RANKS, BLOCK, 2 * DIM)


def collect(grads):
    got = lax.all_to_all(grads.reshape(4 * RANKS, 64, 2 * DIM), PLANE, 0, 0, tiled=True)
    return jnp.sum(got.reshape(RANKS, 4, 64, 2 * DIM).astype(F32), axis=0)


def per_device(queries, key_vectors, value_vectors, out_grad):
    rank = lax.axis_index("ylo") * NX + lax.axis_index("x")
    wide = jnp.where(lax.axis_index("z") % 2 == 0, HALF, 0)
    place = jnp.stack([rank, wide]).astype(jnp.int32)

    block = jnp.transpose(jnp.concatenate([key_vectors, value_vectors], axis=2), (1, 0, 2))
    planes = lax.axis_size("z")
    planes = lax.axis_size("z")
    own = spread(block)

    high = wide == HALF

    def widest(a):
        return jnp.where(high, a[:, HALF:], a[:, :HALF])

    q_next = lax.ppermute(widest(queries), "z", ring(planes, -1))
    g_next = lax.ppermute(widest(out_grad), "z", ring(planes, -1))
    q = jnp.transpose(queries, (1, 0, 2))
    q_t = jnp.transpose(queries, (1, 2, 0))
    g = jnp.transpose(out_grad, (1, 0, 2))
    g_t = jnp.transpose(out_grad, (1, 2, 0))
    q_t_next = jnp.transpose(q_next, (1, 2, 0))
    q_next = jnp.transpose(q_next, (1, 0, 2))
    g_t_next = jnp.transpose(g_next, (1, 2, 0))
    g_next = jnp.transpose(g_next, (1, 0, 2))

    every = HEADS + HALF
    full_t = (HEADS, DIM, BLOCK)
    full = (HEADS, BLOCK, DIM)
    half_t = (HALF, DIM, BLOCK)
    half = (HALF, BLOCK, DIM)
    packed = (HALF, DIM + EXTRA, BLOCK)
    rows = (HEADS, BLOCK)
    few = (HALF, BLOCK)
    square = (HEADS, BLOCK, BLOCK)
    small = (HALF, BLOCK, BLOCK)
    kv_shape = (RANKS, BLOCK, 2 * DIM)
    out_t, mine, nexts, log_narrow, delta_narrow = call(
        forward,
        [(full_t, BF16, FAR), (packed, BF16, FAR), (packed, BF16, FAR), (few, F32, NEAR), (few, F32, NEAR)],
        [(place, None), (own, FAR), (q_t, FAR), (q_t_next, FAR), (g_t, FAR)],
        [
            (kv_shape, BF16), ((every, DIM, BLOCK), BF16), (half_t, BF16), ((every, DIM, BLOCK), F32),
            (half_t, BF16), (packed, BF16), (packed, BF16), ((2 * HEADS, BLOCK), F32), ((2 * HEADS, BLOCK), F32),
            ((every, BLOCK, BLOCK), F32),
        ],
        [4, 3],
        12 << 30,
    )
    before = lax.ppermute(nexts, "z", ring(planes, 1))
    after = lax.ppermute(mine, "z", ring(planes, -1))
    dq_narrow, dkv_narrow = call(
        backward_narrow,
        [(half_t, BF16, FAR), (kv_shape, F32, FAR)],
        [
            (place, None), (own, FAR), (q_t, FAR), (q, FAR), (g_t, FAR), (g, FAR),
            (log_narrow, NEAR), (delta_narrow, NEAR),
        ],
        [
            (kv_shape, BF16), (half_t, BF16), (half, BF16), (half_t, BF16), (half, BF16), (half_t, F32),
            (half_t, BF16), (kv_shape, F32), (small, F32), (small, F32), (small, BF16), (small, BF16),
        ],
        [6, RANKS],
        8 << 30,
    )
    out_t, dq_wide, dq_next, dkv = call(
        backward_wide,
        [(full_t, BF16, FAR), (half_t, BF16, FAR), (half_t, BF16, FAR), (kv_shape, BF16, FAR)],
        [
            (place, None), (own, FAR), (q_t, FAR), (q, FAR), (g_t, FAR), (g, FAR), (q_t_next, FAR), (q_next, FAR),
            (g_t_next, FAR), (g_next, FAR), (mine, FAR), (before, FAR), (nexts, FAR), (after, FAR),
            (dkv_narrow, FAR), (out_t, FAR),
        ],
        [
            (kv_shape, BF16), (full_t, BF16), (full, BF16), (full_t, BF16), (full, BF16),
            (packed, BF16), (packed, BF16), (packed, BF16), (packed, BF16), (kv_shape, F32), (half_t, BF16),
            (full_t, F32), (full_t, BF16), (kv_shape, BF16), (rows, F32), (rows, F32),
            (square, F32), (square, F32), (square, BF16), (square, BF16),
        ],
        [14, 3, RANKS],
        16 << 30,
        {15: 0},
    )
    dq_back = lax.ppermute(dq_next, "z", ring(planes, 1))
    back = jnp.transpose(collect(dkv).astype(BF16), (1, 0, 2))
    attended = jnp.transpose(out_t, (2, 0, 1))
    dq_wide = (dq_wide.astype(F32) + dq_back.astype(F32)).astype(BF16)
    dq_t = jnp.concatenate([jnp.where(high, dq_narrow, dq_wide), jnp.where(high, dq_wide, dq_narrow)], axis=0)
    query_grad = jnp.transpose(dq_t, (2, 0, 1))
    return attended, query_grad, back[:, :, :DIM], back[:, :, DIM:]


def solution(mesh):
    inner = Mesh(mesh.devices.reshape(8, 2, NX, 2, 2), ("z", "ylo", "x", "yhi", "core"))
    tokens = ("z", "ylo", "x")
    heads = ("yhi", "core")
    by_head = P(tokens, heads, None)
    by_token = P(tokens + heads, None, None)
    return jax.shard_map(
        per_device,
        mesh=inner,
        in_specs=(by_head, by_token, by_token, by_head),
        out_specs=(by_head, by_head, by_token, by_token),
        check_vma=False,
    )
```

```python
import math

import jax
import jax.numpy as jnp
from jax import lax
from jax.experimental import pallas as pl
from jax.experimental.pallas import tpu as pltpu
from jax.sharding import Mesh, PartitionSpec as P

BLOCK = 256
DIM = 128
HEADS = 8
HALF = 4
NX = 4
RANKS = 8
TILE = 2 * BLOCK
TILES = RANKS * BLOCK // TILE
EXTRA = 16
LIMIT = 63 << 20
SCALE = 1.0 / math.sqrt(DIM)
TO_LOG2 = SCALE * math.log2(math.e)
F32 = jnp.float32
BF16 = jnp.bfloat16
PLANE = ("ylo", "x", "yhi", "core")


def dot(a, b):
    return jnp.dot(a, b, preferred_element_type=F32)


def causal(place):
    t = lax.broadcasted_iota(jnp.int32, (TILE, BLOCK), 0)
    i = lax.broadcasted_iota(jnp.int32, (TILE, BLOCK), 1)
    return t <= i + lax.rem(place[0], TILE // BLOCK) * BLOCK


def forward_tile(place, kv, lo, hi, q_t, acc, top, total, scores, first, masked):
    key = kv[:, :DIM]
    value_t = kv[:, DIM:].T
    for h in range(lo, hi):
        scores[h] = dot(key, q_t[h])
    for h in range(lo, hi):
        s = scores[h]
        if h < masked:
            s = jnp.where(causal(place), s, -jnp.inf)
        new_top = jnp.max(s, axis=0, keepdims=True)
        if first:
            w = jnp.exp2((s - new_top) * TO_LOG2)
            total[h : h + 1, :] = jnp.sum(w, axis=0, keepdims=True)
            acc[h] = dot(value_t, w.astype(BF16))
        else:
            old_top = top[h : h + 1, :]
            new_top = jnp.maximum(old_top, new_top)
            w = jnp.exp2((s - new_top) * TO_LOG2)
            fade = jnp.exp2((old_top - new_top) * TO_LOG2)
            total[h : h + 1, :] = total[h : h + 1, :] * fade + jnp.sum(w, axis=0, keepdims=True)
            acc[h] = acc[h] * fade + dot(value_t, w.astype(BF16))
        top[h : h + 1, :] = new_top


def backward_tile(
    place, kv, lo, hi, q_t, q, g_t, g, log_total, delta, dq_t, scores, grads, probs, ds, masked, ready=None
):
    key = kv[:, :DIM]
    value = kv[:, DIM:]
    key_t = key.T
    for h in range(lo, hi):
        scores[h] = dot(key, q_t[h])
        grads[h] = dot(value, g_t[h])
    for h in range(lo, hi):
        prob = jnp.exp2(scores[h] * TO_LOG2 - log_total[h : h + 1, :])
        if h < masked:
            prob = jnp.where(causal(place), prob, 0.0)
        probs[h] = prob.astype(BF16)
        ds[h] = (prob * (grads[h] - delta[h : h + 1, :])).astype(BF16)
    if ready is not None:
        ready()
    dv = dot(probs[lo], g[lo])
    dk = dot(ds[lo], q[lo])
    for h in range(lo + 1, hi):
        dv = dv + dot(probs[h], g[h])
        dk = dk + dot(ds[h], q[h])
    for h in range(lo, hi):
        dq_t[h] += dot(key_t, ds[h])
    return jnp.concatenate([dk * SCALE, dv], axis=1)


def finish(o, g_t):
    rounded = o.astype(BF16)
    return rounded, jnp.sum(rounded.astype(F32) * g_t.astype(F32), axis=0, keepdims=True)


def pack(o, log):
    row = lax.broadcasted_iota(jnp.int32, (EXTRA, BLOCK), 0)
    first = log.astype(BF16).astype(F32)
    second = (log - first).astype(BF16).astype(F32)
    third = log - first - second
    tail = jnp.where(row == 0, first, jnp.where(row == 1, second, jnp.where(row == 2, third, 0.0)))
    return jnp.concatenate([o.astype(BF16), tail.astype(BF16)], axis=0)


def log_of(packed):
    return jnp.sum(packed[DIM:].astype(F32), axis=0, keepdims=True)


def merged(a, b):
    log_a = log_of(a)
    log_b = log_of(b)
    top = jnp.maximum(log_a, log_b)
    log = top + jnp.log2(jnp.exp2(log_a - top) + jnp.exp2(log_b - top))
    return a[:DIM].astype(F32) * jnp.exp2(log_a - log) + b[:DIM].astype(F32) * jnp.exp2(log_b - log), log


def start_all(pairs, sems):
    copies = [pltpu.make_async_copy(a, b, sems.at[i]) for i, (a, b) in enumerate(pairs)]
    for copy in copies:
        copy.start()
    return copies


def wait_all(copies):
    for copy in copies:
        copy.wait()


def forward(
    place, kv_in, q_t_in, q_t_next_in, g_t_in,
    out_out, mine_out, next_out, log_narrow, delta_narrow,
    kv, q_t, g_t, acc, out, mine, nexts, top, total, scores, sems, out_sems,
):
    rank = place[0]
    wide = place[1]
    narrow = HALF - wide
    loads = start_all(
        [
            (q_t_in, q_t.at[pl.ds(0, HEADS)]),
            (q_t_next_in, q_t.at[pl.ds(HEADS, HALF)]),
            (kv_in, kv),
            (g_t_in.at[pl.ds(narrow, HALF)], g_t),
        ],
        sems,
    )
    wait_all(loads[:3])
    every = HEADS + HALF
    mine_at = lax.div(rank, TILE // BLOCK)
    forward_tile(place, kv[mine_at], 0, every, q_t, acc, top, total, scores, True, HEADS)

    def below(b, carry):
        forward_tile(place, kv[b], 0, every, q_t, acc, top, total, scores, False, 0)
        return carry

    def above(b, carry):
        forward_tile(place, kv[b], HEADS, every, q_t, acc, top, total, scores, False, 0)
        return carry

    lax.fori_loop(0, mine_at, below, 0)
    lax.fori_loop(mine_at + 1, TILES, above, 0)

    def result(n):
        total_n = total[pl.ds(n, 1), :]
        return acc[n] / total_n, top[pl.ds(n, 1), :] * TO_LOG2 + jnp.log2(total_n)

    for h in range(HALF):
        nexts[h] = pack(*result(HEADS + h))
        mine[h] = pack(*result(wide + h))
    stores = start_all([(nexts, next_out), (mine, mine_out)], out_sems)
    loads[3].wait()
    for h in range(HALF):
        o, log_h = result(narrow + h)
        out[h], delta_narrow[h : h + 1, :] = finish(o, g_t[h])
        log_narrow[h : h + 1, :] = log_h
    last = pltpu.make_async_copy(out, out_out.at[pl.ds(narrow, HALF)], out_sems.at[2])
    last.start()
    wait_all(stores)
    last.wait()


def backward_narrow(
    place, kv_in, q_t_in, q_in, g_t_in, g_in, log_narrow, delta_narrow,
    dq_out, dkv_out,
    kv, q_t, q, g_t, g, dq_t, dq, dkv, scores, grads, probs, ds, sems, tile_sems,
):
    mine_at = lax.div(place[0], TILE // BLOCK)
    part = pl.ds(HALF - place[1], HALF)
    loads = start_all(
        [(q_t_in.at[part], q_t), (kv_in, kv), (g_t_in.at[part], g_t), (g_in.at[part], g), (q_in.at[part], q)],
        sems,
    )
    dq_t[...] = jnp.zeros_like(dq_t)
    wait_all(loads[:3])

    def store(b):
        return pltpu.make_async_copy(dkv.at[b], dkv_out.at[b], tile_sems.at[b])

    def tile(b, masked, ready=None):
        dkv[b] = backward_tile(
            place, kv[b], 0, HALF, q_t, q, g_t, g, log_narrow, delta_narrow, dq_t, scores, grads, probs, ds,
            masked, ready,
        )
        store(b).start()

    tile(mine_at, HALF, lambda: wait_all(loads[3:]))

    def below(b, carry):
        tile(b, 0)
        return carry

    lax.fori_loop(0, mine_at, below, 0)
    dq[...] = (dq_t[...] * SCALE).astype(BF16)
    last = pltpu.make_async_copy(dq, dq_out, sems.at[5])
    last.start()

    def settle(b, carry):
        store(b).wait()
        return carry

    lax.fori_loop(0, mine_at + 1, settle, 0)
    last.wait()


def backward_wide(
    place, kv_in, q_t_in, q_in, g_t_in, g_in, q_t_next_in, g_t_next_in,
    mine_in, before_in, next_in, after_in, dkv_narrow_in, out_in,
    out_out, dq_out, dq_next_out, dkv_out,
    kv, q_t, q, g_t, g, mine, before, nexts, after, dkv_narrow, out, dq_t, dq, dkv, log_total, delta,
    scores, grads, probs, ds, sems, out_sems, tile_sems,
):
    mine_at = lax.div(place[0], TILE // BLOCK)
    part = pl.ds(place[1], HALF)
    first = pl.ds(0, HALF)
    second = pl.ds(HALF, HALF)
    loads = start_all(
        [
            (mine_in, mine), (before_in, before), (g_t_in.at[part], g_t.at[first]),
            (next_in, nexts), (after_in, after), (g_t_next_in, g_t.at[second]),
            (q_t_next_in, q_t.at[second]), (q_t_in.at[part], q_t.at[first]), (kv_in, kv),
            (g_in.at[part], g.at[first]), (q_in.at[part], q.at[first]), (dkv_narrow_in, dkv_narrow),
        ],
        sems,
    )
    dq_t[...] = jnp.zeros_like(dq_t)
    wait_all(loads[:6])
    for h in range(HALF):
        o, log_h = merged(mine[h], before[h])
        out[h], delta[h : h + 1, :] = finish(o, g_t[h])
        log_total[h : h + 1, :] = log_h
        n = HALF + h
        o, log_h = merged(after[h], nexts[h])
        _, delta[n : n + 1, :] = finish(o, g_t[n])
        log_total[n : n + 1, :] = log_h
    out_store = pltpu.make_async_copy(out, out_out.at[part], out_sems.at[0])
    out_store.start()
    wait_all(loads[6:7])
    for n in range(HALF, HEADS):
        q[n] = q_t[n].T
        g[n] = g_t[n].T
    wait_all(loads[7:9])

    def store(b):
        return pltpu.make_async_copy(dkv.at[b], dkv_out.at[b], tile_sems.at[b])

    def tile(b, lo, masked, ready=None):
        grad = backward_tile(
            place, kv[b], lo, HEADS, q_t, q, g_t, g, log_total, delta, dq_t, scores, grads, probs, ds,
            masked, ready,
        )
        if lo == 0:
            grad = grad + dkv_narrow[b]
        dkv[b] = grad.astype(BF16)
        store(b).start()

    tile(mine_at, 0, HALF, lambda: wait_all(loads[9:]))

    def below(b, carry):
        tile(b, 0, 0)
        return carry

    def above(b, carry):
        tile(b, HALF, 0)
        return carry

    lax.fori_loop(0, mine_at, below, 0)
    lax.fori_loop(mine_at + 1, TILES, above, 0)
    dq[...] = (dq_t[...] * SCALE).astype(BF16)
    dq_store = pltpu.make_async_copy(dq.at[first], dq_out, out_sems.at[1])
    dq_next_store = pltpu.make_async_copy(dq.at[second], dq_next_out, out_sems.at[2])
    dq_store.start()
    dq_next_store.start()
    for b in range(TILES):
        store(b).wait()
    out_store.wait()
    dq_store.wait()
    dq_next_store.wait()


FAR = pl.BlockSpec(memory_space=pltpu.HBM)
NEAR = pl.BlockSpec(memory_space=pltpu.VMEM)


def call(body, outs, ins, scratch, sems, flops, aliases=None):
    return pl.pallas_call(
        body,
        out_shape=[jax.ShapeDtypeStruct(s, t) for s, t, _ in outs],
        in_specs=[pl.BlockSpec(memory_space=pltpu.SMEM)] + [spec for _, spec in ins[1:]],
        out_specs=[spec for _, _, spec in outs],
        scratch_shapes=[pltpu.VMEM(s, t) for s, t in scratch] + [pltpu.SemaphoreType.DMA((n,)) for n in sems],
        input_output_aliases=aliases or {},
        compiler_params=pltpu.CompilerParams(vmem_limit_bytes=LIMIT),
        cost_estimate=pl.CostEstimate(flops=flops, bytes_accessed=4 << 20, transcendentals=1 << 20),
    )(*[a for a, _ in ins])


def ring(size, by):
    return [(i, (i + by) % size) for i in range(size)]


def spread(block):
    many = jnp.broadcast_to(block[None], (RANKS,) + block.shape).reshape((4 * RANKS,) + block.shape[1:])
    got = lax.all_to_all(many, PLANE, 0, 0, tiled=True)
    return got.reshape(TILES, TILE, 2 * DIM)


def collect(grads):
    got = lax.all_to_all(grads.reshape(4 * RANKS, 64, 2 * DIM), PLANE, 0, 0, tiled=True)
    return jnp.sum(got.reshape(RANKS, 4, 64, 2 * DIM).astype(F32), axis=0)


def per_device(queries, key_vectors, value_vectors, out_grad):
    rank = lax.axis_index("ylo") * NX + lax.axis_index("x")
    wide = jnp.where(lax.axis_index("z") % 2 == 0, HALF, 0)
    place = jnp.stack([rank, wide]).astype(jnp.int32)

    block = jnp.transpose(jnp.concatenate([key_vectors, value_vectors], axis=2), (1, 0, 2))
    planes = lax.axis_size("z")
    planes = lax.axis_size("z")
    own = spread(block)

    high = wide == HALF

    q = jnp.transpose(queries, (1, 0, 2))
    q_t = jnp.transpose(queries, (1, 2, 0))
    g = jnp.transpose(out_grad, (1, 0, 2))
    g_t = jnp.transpose(out_grad, (1, 2, 0))

    def widest(a):
        return jnp.where(high, a[HALF:], a[:HALF])

    q_t_next = lax.ppermute(widest(q_t), "z", ring(planes, -1))
    g_t_next = lax.ppermute(widest(g_t), "z", ring(planes, -1))

    every = HEADS + HALF
    full_t = (HEADS, DIM, BLOCK)
    full = (HEADS, BLOCK, DIM)
    half_t = (HALF, DIM, BLOCK)
    half = (HALF, BLOCK, DIM)
    packed = (HALF, DIM + EXTRA, BLOCK)
    rows = (HEADS, BLOCK)
    few = (HALF, BLOCK)
    square = (HEADS, TILE, BLOCK)
    small = (HALF, TILE, BLOCK)
    kv_shape = (TILES, TILE, 2 * DIM)
    out_t, mine, nexts, log_narrow, delta_narrow = call(
        forward,
        [(full_t, BF16, FAR), (packed, BF16, FAR), (packed, BF16, FAR), (few, F32, NEAR), (few, F32, NEAR)],
        [(place, None), (own, FAR), (q_t, FAR), (q_t_next, FAR), (g_t, FAR)],
        [
            (kv_shape, BF16), ((every, DIM, BLOCK), BF16), (half_t, BF16), ((every, DIM, BLOCK), F32),
            (half_t, BF16), (packed, BF16), (packed, BF16), ((2 * HEADS, BLOCK), F32), ((2 * HEADS, BLOCK), F32),
            ((every, TILE, BLOCK), F32),
        ],
        [4, 3],
        12 << 30,
    )
    before = lax.ppermute(nexts, "z", ring(planes, 1))
    after = lax.ppermute(mine, "z", ring(planes, -1))
    dq_narrow, dkv_narrow = call(
        backward_narrow,
        [(half_t, BF16, FAR), (kv_shape, F32, FAR)],
        [
            (place, None), (own, FAR), (q_t, FAR), (q, FAR), (g_t, FAR), (g, FAR),
            (log_narrow, NEAR), (delta_narrow, NEAR),
        ],
        [
            (kv_shape, BF16), (half_t, BF16), (half, BF16), (half_t, BF16), (half, BF16), (half_t, F32),
            (half_t, BF16), (kv_shape, F32), (small, F32), (small, F32), (small, BF16), (small, BF16),
        ],
        [6, TILES],
        8 << 30,
    )
    out_t, dq_wide, dq_next, dkv = call(
        backward_wide,
        [(full_t, BF16, FAR), (half_t, BF16, FAR), (half_t, BF16, FAR), (kv_shape, BF16, FAR)],
        [
            (place, None), (own, FAR), (q_t, FAR), (q, FAR), (g_t, FAR), (g, FAR), (q_t_next, FAR),
            (g_t_next, FAR), (mine, FAR), (before, FAR), (nexts, FAR), (after, FAR),
            (dkv_narrow, FAR), (out_t, FAR),
        ],
        [
            (kv_shape, BF16), (full_t, BF16), (full, BF16), (full_t, BF16), (full, BF16),
            (packed, BF16), (packed, BF16), (packed, BF16), (packed, BF16), (kv_shape, F32), (half_t, BF16),
            (full_t, F32), (full_t, BF16), (kv_shape, BF16), (rows, F32), (rows, F32),
            (square, F32), (square, F32), (square, BF16), (square, BF16),
        ],
        [12, 3, TILES],
        16 << 30,
        {13: 0},
    )
    dq_back = lax.ppermute(dq_next, "z", ring(planes, 1))
    back = jnp.transpose(collect(dkv).astype(BF16), (1, 0, 2))
    attended = jnp.transpose(out_t, (2, 0, 1))
    dq_wide = (dq_wide.astype(F32) + dq_back.astype(F32)).astype(BF16)
    dq_t = jnp.concatenate([jnp.where(high, dq_narrow, dq_wide), jnp.where(high, dq_wide, dq_narrow)], axis=0)
    query_grad = jnp.transpose(dq_t, (2, 0, 1))
    return attended, query_grad, back[:, :, :DIM], back[:, :, DIM:]


def solution(mesh):
    inner = Mesh(mesh.devices.reshape(8, 2, NX, 2, 2), ("z", "ylo", "x", "yhi", "core"))
    tokens = ("z", "ylo", "x")
    heads = ("yhi", "core")
    by_head = P(tokens, heads, None)
    by_token = P(tokens + heads, None, None)
    return jax.shard_map(
        per_device,
        mesh=inner,
        in_specs=(by_head, by_token, by_token, by_head),
        out_specs=(by_head, by_head, by_token, by_token),
        check_vma=False,
    )
```

```python
import math

import jax
import jax.numpy as jnp
from jax import lax
from jax.experimental import pallas as pl
from jax.experimental.pallas import tpu as pltpu
from jax.sharding import Mesh, PartitionSpec as P

BLOCK = 256
DIM = 128
HEADS = 8
HALF = 4
NX = 4
RANKS = 8
TILE = 2 * BLOCK
TILES = RANKS * BLOCK // TILE
EXTRA = 16
LIMIT = 63 << 20
SCALE = 1.0 / math.sqrt(DIM)
TO_LOG2 = SCALE * math.log2(math.e)
F32 = jnp.float32
BF16 = jnp.bfloat16
PLANE = ("ylo", "x", "yhi", "core")


def dot(a, b):
    return jnp.dot(a, b, preferred_element_type=F32)


def causal(place):
    t = lax.broadcasted_iota(jnp.int32, (TILE, BLOCK), 0)
    i = lax.broadcasted_iota(jnp.int32, (TILE, BLOCK), 1)
    return t <= i + lax.rem(place[0], TILE // BLOCK) * BLOCK


def forward_tile(place, kv, lo, hi, q_t, acc, top, total, scores, first, masked):
    key = kv[:, :DIM]
    value_t = kv[:, DIM:].T
    for h in range(lo, hi):
        scores[h] = dot(key, q_t[h])
    for h in range(lo, hi):
        s = scores[h]
        if h < masked:
            s = jnp.where(causal(place), s, -jnp.inf)
        new_top = jnp.max(s, axis=0, keepdims=True)
        if first:
            w = jnp.exp2((s - new_top) * TO_LOG2)
            total[h : h + 1, :] = jnp.sum(w, axis=0, keepdims=True)
            acc[h] = dot(value_t, w.astype(BF16))
        else:
            old_top = top[h : h + 1, :]
            new_top = jnp.maximum(old_top, new_top)
            w = jnp.exp2((s - new_top) * TO_LOG2)
            fade = jnp.exp2((old_top - new_top) * TO_LOG2)
            total[h : h + 1, :] = total[h : h + 1, :] * fade + jnp.sum(w, axis=0, keepdims=True)
            acc[h] = acc[h] * fade + dot(value_t, w.astype(BF16))
        top[h : h + 1, :] = new_top


def backward_tile(
    place, kv, lo, hi, q_t, q, g_t, g, log_total, delta, dq_t, scores, grads, probs, ds, masked,
    ready=None,
):
    key = kv[:, :DIM]
    value = kv[:, DIM:]
    key_t = key.T
    for h in range(lo, hi):
        scores[h] = dot(key, q_t[h])
        grads[h] = dot(value, g_t[h])
    for h in range(lo, hi):
        prob = jnp.exp2(scores[h] * TO_LOG2 - log_total[h : h + 1, :])
        if h < masked:
            prob = jnp.where(causal(place), prob, 0.0)
        probs[h] = prob.astype(BF16)
        ds[h] = (prob * (grads[h] - delta[h : h + 1, :])).astype(BF16)
    if ready is not None:
        ready()
    dv = dot(probs[lo], g[lo])
    dk = dot(ds[lo], q[lo])
    for h in range(lo + 1, hi):
        dv = dv + dot(probs[h], g[h])
        dk = dk + dot(ds[h], q[h])
    for h in range(lo, hi):
        dq_t[h] += dot(key_t, ds[h])
    return jnp.concatenate([dk * SCALE, dv], axis=1)


def finish(o, g_t):
    rounded = o.astype(BF16)
    return rounded, jnp.sum(rounded.astype(F32) * g_t.astype(F32), axis=0, keepdims=True)


def pack(o, log):
    row = lax.broadcasted_iota(jnp.int32, (EXTRA, BLOCK), 0)
    first = log.astype(BF16).astype(F32)
    second = (log - first).astype(BF16).astype(F32)
    third = log - first - second
    tail = jnp.where(row == 0, first, jnp.where(row == 1, second, jnp.where(row == 2, third, 0.0)))
    return jnp.concatenate([o.astype(BF16), tail.astype(BF16)], axis=0)


def log_of(packed):
    return jnp.sum(packed[DIM:].astype(F32), axis=0, keepdims=True)


def merged(a, b):
    log_a = log_of(a)
    log_b = log_of(b)
    top = jnp.maximum(log_a, log_b)
    log = top + jnp.log2(jnp.exp2(log_a - top) + jnp.exp2(log_b - top))
    return a[:DIM].astype(F32) * jnp.exp2(log_a - log) + b[:DIM].astype(F32) * jnp.exp2(log_b - log), log


def start_all(pairs, sems):
    copies = [pltpu.make_async_copy(a, b, sems.at[i]) for i, (a, b) in enumerate(pairs)]
    for copy in copies:
        copy.start()
    return copies


def wait_all(copies):
    for copy in copies:
        copy.wait()


def forward(
    place, kv_in, q_t_in, q_t_next_in,
    mine_out, next_out, narrow_out,
    kv, q_t, acc, mine, nexts, narrows, top, total, scores, sems, out_sems,
):
    rank = place[0]
    wide = place[1]
    narrow = HALF - wide
    loads = start_all(
        [
            (q_t_in, q_t.at[pl.ds(0, HEADS)]),
            (q_t_next_in, q_t.at[pl.ds(HEADS, HALF)]),
            (kv_in, kv),
        ],
        sems,
    )
    wait_all(loads)
    every = HEADS + HALF
    mine_at = lax.div(rank, TILE // BLOCK)
    forward_tile(place, kv[mine_at], 0, every, q_t, acc, top, total, scores, True, HEADS)

    def below(b, carry):
        forward_tile(place, kv[b], 0, every, q_t, acc, top, total, scores, False, 0)
        return carry

    def above(b, carry):
        forward_tile(place, kv[b], HEADS, every, q_t, acc, top, total, scores, False, 0)
        return carry

    lax.fori_loop(0, mine_at, below, 0)
    lax.fori_loop(mine_at + 1, TILES, above, 0)

    def result(n):
        total_n = total[pl.ds(n, 1), :]
        return acc[n] / total_n, top[pl.ds(n, 1), :] * TO_LOG2 + jnp.log2(total_n)

    for h in range(HALF):
        nexts[h] = pack(*result(HEADS + h))
        mine[h] = pack(*result(wide + h))
        narrows[h] = pack(*result(narrow + h))
    wait_all(start_all([(nexts, next_out), (mine, mine_out), (narrows, narrow_out)], out_sems))


def backward_narrow(
    place, kv_in, q_t_in, q_in, g_t_in, g_in, packed_in,
    out_out, dq_out, dkv_out,
    kv, q_t, q, g_t, g, packed, out, dq_t, dq, dkv, log_narrow, delta_narrow, scores, grads, probs, ds,
    sems, out_sems, tile_sems,
):
    mine_at = lax.div(place[0], TILE // BLOCK)
    part = pl.ds(HALF - place[1], HALF)
    loads = start_all(
        [
            (packed_in, packed), (g_t_in.at[part], g_t), (q_t_in.at[part], q_t), (kv_in, kv),
            (g_in.at[part], g), (q_in.at[part], q),
        ],
        sems,
    )
    out_store = pltpu.make_async_copy(out, out_out.at[part], out_sems.at[0])

    dq_t[...] = jnp.zeros_like(dq_t)
    wait_all(loads[:2])
    for h in range(HALF):
        out[h], delta_narrow[h : h + 1, :] = finish(packed[h, :DIM].astype(F32), g_t[h])
        log_narrow[h : h + 1, :] = log_of(packed[h])
    out_store.start()
    wait_all(loads[2:4])

    def store(b):
        return pltpu.make_async_copy(dkv.at[b], dkv_out.at[b], tile_sems.at[b])

    def tile(b, masked, ready=None):
        dkv[b] = backward_tile(
            place, kv[b], 0, HALF, q_t, q, g_t, g, log_narrow, delta_narrow, dq_t, scores, grads, probs, ds,
            masked, ready,
        )
        store(b).start()

    tile(mine_at, HALF, lambda: wait_all(loads[4:]))

    def below(b, carry):
        tile(b, 0)
        return carry

    lax.fori_loop(0, mine_at, below, 0)
    dq[...] = (dq_t[...] * SCALE).astype(BF16)
    last = pltpu.make_async_copy(dq, dq_out, out_sems.at[1])
    last.start()

    def settle(b, carry):
        store(b).wait()
        return carry

    lax.fori_loop(0, mine_at + 1, settle, 0)
    last.wait()
    out_store.wait()


def backward_wide(
    place, kv_in, q_t_in, q_in, g_t_in, g_in, q_t_next_in, g_t_next_in,
    mine_in, before_in, next_in, after_in, dkv_narrow_in, out_in,
    out_out, dq_out, dq_next_out, dkv_out,
    kv, q_t, q, g_t, g, mine, before, nexts, after, dkv_narrow, out, dq_t, dq, dkv, log_total, delta,
    scores, grads, probs, ds, sems, out_sems, tile_sems,
):
    mine_at = lax.div(place[0], TILE // BLOCK)
    part = pl.ds(place[1], HALF)
    first = pl.ds(0, HALF)
    second = pl.ds(HALF, HALF)
    loads = start_all(
        [
            (mine_in, mine), (before_in, before), (g_t_in.at[part], g_t.at[first]),
            (next_in, nexts), (after_in, after), (g_t_next_in, g_t.at[second]),
            (q_t_next_in, q_t.at[second]), (q_t_in.at[part], q_t.at[first]), (kv_in, kv),
            (g_in.at[part], g.at[first]), (q_in.at[part], q.at[first]), (dkv_narrow_in, dkv_narrow),
        ],
        sems,
    )
    dq_t[...] = jnp.zeros_like(dq_t)
    wait_all(loads[:6])
    for h in range(HALF):
        o, log_h = merged(mine[h], before[h])
        out[h], delta[h : h + 1, :] = finish(o, g_t[h])
        log_total[h : h + 1, :] = log_h
        n = HALF + h
        o, log_h = merged(after[h], nexts[h])
        _, delta[n : n + 1, :] = finish(o, g_t[n])
        log_total[n : n + 1, :] = log_h
    out_store = pltpu.make_async_copy(out, out_out.at[part], out_sems.at[0])
    out_store.start()
    wait_all(loads[6:7])
    for n in range(HALF, HEADS):
        q[n] = q_t[n].T
        g[n] = g_t[n].T
    wait_all(loads[7:9])

    def store(b):
        return pltpu.make_async_copy(dkv.at[b], dkv_out.at[b], tile_sems.at[b])

    def tile(b, lo, masked, ready=None):
        grad = backward_tile(
            place, kv[b], lo, HEADS, q_t, q, g_t, g, log_total, delta, dq_t, scores, grads, probs, ds,
            masked, ready,
        )
        if lo == 0:
            grad = grad + dkv_narrow[b]
        dkv[b] = grad.astype(BF16)
        store(b).start()

    tile(mine_at, 0, HALF, lambda: wait_all(loads[9:]))

    def below(b, carry):
        tile(b, 0, 0)
        return carry

    def above(b, carry):
        tile(b, HALF, 0)
        return carry

    lax.fori_loop(0, mine_at, below, 0)
    lax.fori_loop(mine_at + 1, TILES, above, 0)
    dq[...] = (dq_t[...] * SCALE).astype(BF16)
    dq_store = pltpu.make_async_copy(dq.at[first], dq_out, out_sems.at[1])
    dq_next_store = pltpu.make_async_copy(dq.at[second], dq_next_out, out_sems.at[2])
    dq_store.start()
    dq_next_store.start()
    for b in range(TILES):
        store(b).wait()
    out_store.wait()
    dq_store.wait()
    dq_next_store.wait()


FAR = pl.BlockSpec(memory_space=pltpu.HBM)
NEAR = pl.BlockSpec(memory_space=pltpu.VMEM)


def call(body, outs, ins, scratch, sems, flops, aliases=None):
    return pl.pallas_call(
        body,
        out_shape=[jax.ShapeDtypeStruct(s, t) for s, t, _ in outs],
        in_specs=[pl.BlockSpec(memory_space=pltpu.SMEM)] + [spec for _, spec in ins[1:]],
        out_specs=[spec for _, _, spec in outs],
        scratch_shapes=[pltpu.VMEM(s, t) for s, t in scratch] + [pltpu.SemaphoreType.DMA((n,)) for n in sems],
        input_output_aliases=aliases or {},
        compiler_params=pltpu.CompilerParams(vmem_limit_bytes=LIMIT),
        cost_estimate=pl.CostEstimate(flops=flops, bytes_accessed=4 << 20, transcendentals=1 << 20),
    )(*[a for a, _ in ins])


def ring(size, by):
    return [(i, (i + by) % size) for i in range(size)]


def spread(block):
    many = jnp.broadcast_to(block[None], (RANKS,) + block.shape).reshape((4 * RANKS,) + block.shape[1:])
    got = lax.all_to_all(many, PLANE, 0, 0, tiled=True)
    return got.reshape(TILES, TILE, 2 * DIM)


def collect(grads):
    got = lax.all_to_all(grads.reshape(4 * RANKS, 64, 2 * DIM), PLANE, 0, 0, tiled=True)
    return jnp.sum(got.reshape(RANKS, 4, 64, 2 * DIM).astype(F32), axis=0)


def per_device(queries, key_vectors, value_vectors, out_grad):
    rank = lax.axis_index("ylo") * NX + lax.axis_index("x")
    wide = jnp.where(lax.axis_index("z") % 2 == 0, HALF, 0)
    place = jnp.stack([rank, wide]).astype(jnp.int32)

    block = jnp.transpose(jnp.concatenate([key_vectors, value_vectors], axis=2), (1, 0, 2))
    planes = lax.axis_size("z")
    planes = lax.axis_size("z")
    own = spread(block)

    high = wide == HALF

    q = jnp.transpose(queries, (1, 0, 2))
    q_t = jnp.transpose(queries, (1, 2, 0))
    g = jnp.transpose(out_grad, (1, 0, 2))
    g_t = jnp.transpose(out_grad, (1, 2, 0))

    def widest(a):
        return jnp.where(high, a[HALF:], a[:HALF])

    q_t_next = lax.ppermute(widest(q_t), "z", ring(planes, -1))
    g_t_next = lax.ppermute(widest(g_t), "z", ring(planes, -1))

    every = HEADS + HALF
    full_t = (HEADS, DIM, BLOCK)
    full = (HEADS, BLOCK, DIM)
    half_t = (HALF, DIM, BLOCK)
    half = (HALF, BLOCK, DIM)
    packed = (HALF, DIM + EXTRA, BLOCK)
    rows = (HEADS, BLOCK)
    few = (HALF, BLOCK)
    square = (HEADS, TILE, BLOCK)
    small = (HALF, TILE, BLOCK)
    kv_shape = (TILES, TILE, 2 * DIM)
    mine, nexts, narrows = call(
        forward,
        [(packed, BF16, FAR), (packed, BF16, FAR), (packed, BF16, FAR)],
        [(place, None), (own, FAR), (q_t, FAR), (q_t_next, FAR)],
        [
            (kv_shape, BF16), ((every, DIM, BLOCK), BF16), ((every, DIM, BLOCK), F32),
            (packed, BF16), (packed, BF16), (packed, BF16), ((2 * HEADS, BLOCK), F32), ((2 * HEADS, BLOCK), F32),
            ((every, TILE, BLOCK), F32),
        ],
        [3, 3],
        12 << 30,
    )
    before = lax.ppermute(nexts, "z", ring(planes, 1))
    after = lax.ppermute(mine, "z", ring(planes, -1))
    out_t, dq_narrow, dkv_narrow = call(
        backward_narrow,
        [(full_t, BF16, FAR), (half_t, BF16, FAR), (kv_shape, F32, FAR)],
        [(place, None), (own, FAR), (q_t, FAR), (q, FAR), (g_t, FAR), (g, FAR), (narrows, FAR)],
        [
            (kv_shape, BF16), (half_t, BF16), (half, BF16), (half_t, BF16), (half, BF16), (packed, BF16),
            (half_t, BF16), (half_t, F32), (half_t, BF16), (kv_shape, F32), (few, F32), (few, F32),
            (small, F32), (small, F32), (small, BF16), (small, BF16),
        ],
        [6, 2, TILES],
        8 << 30,
    )
    out_t, dq_wide, dq_next, dkv = call(
        backward_wide,
        [(full_t, BF16, FAR), (half_t, BF16, FAR), (half_t, BF16, FAR), (kv_shape, BF16, FAR)],
        [
            (place, None), (own, FAR), (q_t, FAR), (q, FAR), (g_t, FAR), (g, FAR), (q_t_next, FAR),
            (g_t_next, FAR), (mine, FAR), (before, FAR), (nexts, FAR), (after, FAR),
            (dkv_narrow, FAR), (out_t, FAR),
        ],
        [
            (kv_shape, BF16), (full_t, BF16), (full, BF16), (full_t, BF16), (full, BF16),
            (packed, BF16), (packed, BF16), (packed, BF16), (packed, BF16), (kv_shape, F32), (half_t, BF16),
            (full_t, F32), (full_t, BF16), (kv_shape, BF16), (rows, F32), (rows, F32),
            (square, F32), (square, F32), (square, BF16), (square, BF16),
        ],
        [12, 3, TILES],
        16 << 30,
        {13: 0},
    )
    dq_back = lax.ppermute(dq_next, "z", ring(planes, 1))
    back = jnp.transpose(collect(dkv).astype(BF16), (1, 0, 2))
    attended = jnp.transpose(out_t, (2, 0, 1))
    dq_wide = (dq_wide.astype(F32) + dq_back.astype(F32)).astype(BF16)
    dq_t = jnp.concatenate([jnp.where(high, dq_narrow, dq_wide), jnp.where(high, dq_wide, dq_narrow)], axis=0)
    query_grad = jnp.transpose(dq_t, (2, 0, 1))
    return attended, query_grad, back[:, :, :DIM], back[:, :, DIM:]


def solution(mesh):
    inner = Mesh(mesh.devices.reshape(8, 2, NX, 2, 2), ("z", "ylo", "x", "yhi", "core"))
    tokens = ("z", "ylo", "x")
    heads = ("yhi", "core")
    by_head = P(tokens, heads, None)
    by_token = P(tokens + heads, None, None)
    return jax.shard_map(
        per_device,
        mesh=inner,
        in_specs=(by_head, by_token, by_token, by_head),
        out_specs=(by_head, by_head, by_token, by_token),
        check_vma=False,
    )
```
